256 devices in a mesh: aa: 8 (over y, core), ba: 4 (over x), col: 8 (over z).
Axes of the slice: x: 4, y: 4, z: 8, core: 2. Of those that a mesh axis runs over, the one named last changes fastest.
Arguments:
- hidden: bfloat16 [8, 4, 32, 8192], P('aa', 'ba', None, 'col'), may hold values from -36 to 60, as said below
- unembed: bfloat16 [8192, 152064], P(None, ('aa', 'ba', 'col')), may hold values from -1 to 5, as said below
- targets: int32 [8, 4, 32], replicated, may hold values from 0 to 152063
- lengths: int32 [8, 4], replicated, may hold values from 1 to 32
Outputs:
- scores: float32 [8, 4], P('aa', 'ba')
The draws below stay inside these ranges and needn't reach their ends.
Inputs may be any that keep to these rules, and one draw needn't show every extreme that they name: real-valued hidden states. `unembed`: real-valued unembedding entries.
All inputs are finite; a program needn't handle non-finite values.
Results may differ from the reference program's by a relative error of at most 0.0003.
Values may be sent and summed in bfloat16 or wider, within the bound.
A program may use at most 128 MiB of HBM per device.

```python
import jax
import jax.numpy as jnp

D = 8192
VOCAB = 152064
CHOICES = 4
LEN = 32
QUEST = 8


def draw_unembed(key, part):
    base = jax.random.truncated_normal(key, -6.0, 6.0, (D, VOCAB), jnp.float32) * D ** (-0.5)
    return base.astype(jnp.bfloat16)


def draw_hidden(key, part):
    shape = (QUEST, CHOICES, LEN, D)
    base = 3.0 * jax.random.truncated_normal(key, -8.0, 8.0, shape, jnp.float32)
    return base.astype(jnp.bfloat16)


def with_ends(result, own_key, low, top_value):
    longest = result.shape.index(max(result.shape))
    spots = []
    for shift in (0, 1):
        where = [jax.random.randint(jax.random.fold_in(own_key, axis), (), 0, length) for axis, length in enumerate(result.shape)]
        where[longest] = (where[longest] + shift) % result.shape[longest]
        spots.append(tuple(where))
    return result.at[spots[0]].set(low).at[spots[1]].set(top_value)


def setup_inputs(seed: int = 0) -> dict:
    key_list = jax.random.split(jax.random.key(seed), 5)
    hidden = draw_hidden(jax.random.fold_in(key_list[4], 71), 0)
    unembed = draw_unembed(jax.random.fold_in(key_list[4], 71), 0)
    targets = with_ends(jax.random.randint(key_list[2], (QUEST, CHOICES, LEN), 0, VOCAB), jax.random.fold_in(key_list[2], 1), 0, VOCAB - 1).astype(jnp.int32)
    lengths = with_ends(jax.random.randint(key_list[3], (QUEST, CHOICES), 1, LEN + 1), jax.random.fold_in(key_list[3], 1), 1, LEN).astype(jnp.int32)
    return dict(hidden=hidden, unembed=unembed, targets=targets, lengths=lengths)


def reference(hidden, unembed, targets, lengths):
    rows = hidden.reshape(-1, D)
    logits = jnp.dot(rows, unembed, preferred_element_type=jnp.float32)
    top = jnp.max(logits, axis=1)
    total = jnp.sum(jnp.exp(logits - top[:, None]), axis=1)
    picked = jnp.take_along_axis(logits, targets.reshape(-1, 1).astype(jnp.int32), axis=1)[:, 0]
    logprob = (picked - top - jnp.log(total)).reshape(QUEST, CHOICES, LEN)
    positions = jnp.arange(LEN, dtype=jnp.int32)
    valid = positions[None, None, :] < lengths[:, :, None]
    summed = jnp.sum(jnp.where(valid, logprob, jnp.zeros_like(logprob)), axis=2)
    return summed / lengths.astype(jnp.float32)
```

```python
import functools

import jax
import jax.numpy as jnp
from jax import lax
from jax.experimental import pallas as pl
from jax.experimental.pallas import tpu as pltpu
from jax.sharding import PartitionSpec as P

MESH = pl.DeviceIdType.MESH
NX, NY, NZ, NC = 4, 4, 8, 2
SEQ = 32
WIDE, THIN = 768, 256
WAVES = NZ
BF16, F32 = jnp.bfloat16, jnp.float32


def kernel(
    hid, unembed, targets, lengths, out,
    hab, hc, ub, acc, tcol, stat, gath, zst,
    own_sem, usem, zr, zs, pr, ps, tr, ts, dr, ds, cr, cs, er, es,
):
    aa, x, z = lax.axis_index("aa"), lax.axis_index("ba"), lax.axis_index("col")
    y, c = aa // 2, aa % 2
    vocab = unembed.shape[1]
    other = 1 - c

    def at(xx, yy, zz, cc):
        return {"aa": yy * 2 + cc, "ba": xx, "col": zz}

    xp, xm = (x + 1) % NX, (x + NX - 1) % NX
    yp, ym = (y + 1) % NY, (y + NY - 1) % NY
    zp, zm = (z + 1) % NZ, (z + NZ - 1) % NZ
    to_xp, to_xm = at(xp, y, z, c), at(xm, y, z, c)
    to_yp, to_ym = at(x, yp, z, c), at(x, ym, z, c)
    to_zp, to_zm = at(x, y, zp, c), at(x, y, zm, c)
    partner = at(x, y, z, other)

    def copy(src, dst, ssem, rsem, dev):
        return pltpu.make_async_remote_copy(
            src_ref=src, dst_ref=dst, send_sem=ssem, recv_sem=rsem, device_id=dev, device_id_type=MESH
        )

    def push(ref, ssem, rsem, dev):
        copy(ref, ref, ssem, rsem, dev).start()

    def got(ref, ssem, rsem):
        copy(ref, ref, ssem, rsem, partner).wait_recv()

    def sent(ref, ssem, rsem):
        copy(ref, ref, ssem, rsem, partner).wait_send()

    wide_in = pltpu.make_async_copy(
        hid.at[0, 0, :, pl.ds(0, WIDE)], hab.at[z, c, x, y], own_sem.at[0])
    thin_in = pltpu.make_async_copy(
        hid.at[0, 0, :, pl.ds(WIDE, THIN)], hc.at[z, c, x, y], own_sem.at[1])
    wide_in.start()
    thin_in.start()

    def weights(k):
        return pltpu.make_async_copy(
            unembed.at[pl.ds(k * 1024, 1024), :], ub.at[k], usem.at[k])

    barrier = pltpu.get_barrier_semaphore()
    for dev in (to_xp, to_xm, to_yp, to_ym, to_zp, to_zm, partner):
        pl.semaphore_signal(barrier, inc=1, device_id=dev, device_id_type=MESH)
    wide_in.wait()
    thin_in.wait()
    pl.semaphore_wait(barrier, 7)

    def s1(b, zz, wa, w):
        s, r = ps.at[w, 0], pr.at[w, 0]
        one = b.at[zz, c, x, y, :, pl.ds(0, wa)]
        two = b.at[zz, c, x, y, :, pl.ds(wa, wa)]
        push(one, s, r, to_yp)
        push(two, s, r, to_xp)
        push(one, s, r, to_ym)
        push(two, s, r, to_xm)

    def s2(b, zz, wa, w):
        got(b.at[zz, c, x, :, :, pl.ds(0, wa)], ps.at[w, 0], pr.at[w, 0])
        s, r = ps.at[w, 1], pr.at[w, 1]
        push(b.at[zz, c, x, ym, pl.ds(0, 16), pl.ds(0, wa)], s, r, to_yp)
        push(b.at[zz, c, xm, y, pl.ds(0, 16), pl.ds(wa, wa)], s, r, to_xp)
        push(b.at[zz, c, x, yp, pl.ds(16, 16), pl.ds(0, wa)], s, r, to_ym)
        push(b.at[zz, c, xp, y, pl.ds(16, 16), pl.ds(wa, wa)], s, r, to_xm)

    def s3(b, zz, wa, w):
        got(b.at[zz, c, x, pl.ds(0, 2), :, pl.ds(0, wa)], ps.at[w, 1], pr.at[w, 1])
        s, r = ps.at[w, 2], pr.at[w, 2]
        one = b.at[zz, c, x, :, :, pl.ds(0, wa)]
        two = b.at[zz, c, :, y, :, pl.ds(wa, wa)]
        push(one, s, r, to_xp)
        push(two, s, r, to_yp)
        push(one, s, r, to_xm)
        push(two, s, r, to_ym)

    def s4(b, zz, wa, w):
        got(b.at[zz, c, :, :, :, pl.ds(0, wa)], ps.at[w, 2], pr.at[w, 2])
        s, r = ps.at[w, 3], pr.at[w, 3]
        push(b.at[zz, c, xm, pl.ds(0, 2), :, pl.ds(0, wa)], s, r, to_xp)
        push(b.at[zz, c, pl.ds(0, 2), ym, :, pl.ds(wa, wa)], s, r, to_yp)
        push(b.at[zz, c, xp, pl.ds(2, 2), :, pl.ds(0, wa)], s, r, to_xm)
        push(b.at[zz, c, pl.ds(2, 2), yp, :, pl.ds(wa, wa)], s, r, to_ym)

    def s5(b, zz, wa, w):
        got(b.at[zz, c, pl.ds(0, 2), :, :, pl.ds(0, wa)], ps.at[w, 3], pr.at[w, 3])

    def s_done(b, wa, w):
        sent(b.at[0, 0, 0, :, :, pl.ds(0, wa)], ps.at[w, 0], pr.at[w, 0])
        sent(b.at[0, 0, 0, pl.ds(0, 2), :, pl.ds(0, wa)], ps.at[w, 1], pr.at[w, 1])
        sent(b.at[0, 0, :, :, :, pl.ds(0, wa)], ps.at[w, 2], pr.at[w, 2])
        sent(b.at[0, 0, pl.ds(0, 2), :, :, pl.ds(0, wa)], ps.at[w, 3], pr.at[w, 3])

    def slot(j):
        k = (j + 1) // 2
        return (z + NZ + k * (1 - 2 * (j % 2))) % NZ

    LAST = WAVES
    wa, wc = WIDE // 2, THIN // 2

    def z_in(j):
        got(hab.at[slot(j), c, x, y], zs.at[j], zr.at[j])

    def z_on(j):
        @pl.when(j == 0)
        def _():
            push(hab.at[z, c, x, y], zs.at[1], zr.at[1], to_zp)
            push(hab.at[z, c, x, y], zs.at[2], zr.at[2], to_zm)

        @pl.when((j % 2 == 1) & (j < WAVES - 1))
        def _():
            push(hab.at[slot(j), c, x, y], zs.at[j + 2], zr.at[j + 2], to_zp)

        @pl.when((j % 2 == 0) & (j > 0) & (j < WAVES - 2))
        def _():
            push(hab.at[slot(j), c, x, y], zs.at[j + 2], zr.at[j + 2], to_zm)

    def t1():
        for q in range(2):
            mine = hc.at[z, c, pl.ds(2 * q, 2)]
            push(mine, ts.at[0, q], tr.at[0, q], to_zp)
            push(mine, ts.at[0, q], tr.at[0, q], to_zm)

    def t_in(k, q):
        got(hc.at[z, c], ts.at[k - 1, q], tr.at[k - 1, q])

    def t_step(k, q):
        t_in(k, q)
        below, above = (z + NZ - k) % NZ, (z + k) % NZ
        if k < 3:
            push(hc.at[below, c, pl.ds(2 * q, 2)], ts.at[k, q], tr.at[k, q], to_zp)
            push(hc.at[above, c, pl.ds(2 * q, 2)], ts.at[k, q], tr.at[k, q], to_zm)
        elif q == 0:
            push(hc.at[below, c, pl.ds(0, 2)], ts.at[3, 0], tr.at[3, 0], to_zp)
        else:
            push(hc.at[above, c, pl.ds(2, 2)], ts.at[3, 0], tr.at[3, 0], to_zm)

    def thin_over(k):
        push(hc.at[(z + NZ - k) % NZ, c], cs.at[k], cr.at[k], partner)
        if 0 < k < 4:
            push(hc.at[(z + k) % NZ, c], cs.at[k], cr.at[k], partner)

    def thin_bytes(k):
        return hc.at[0] if 0 < k < 4 else hc.at[0, 0]

    def multiply(b, zz, k0, kw):
        @pl.loop(0, NC)
        def _(h):
            lhs = b[zz, h].reshape(NX * NY * SEQ, kw)
            rhs = ub[zz, pl.ds(k0, kw), :]
            rows = pl.ds(pl.multiple_of(h * 512, 512), 512)
            acc[rows, :] += jnp.dot(lhs, rhs, preferred_element_type=F32)

    def thin_multiply(k):
        got(thin_bytes(k), cs.at[k], cr.at[k])
        multiply(hc, (z + NZ - k) % NZ, WIDE, THIN)
        if 0 < k < 4:
            multiply(hc, (z + k) % NZ, WIDE, THIN)

    s1(hc, z, wc, LAST)
    z_on(0)
    s1(hab, z, wa, 0)

    for k in range(NZ):
        weights(k).start()
    acc[...] = jnp.zeros_like(acc)
    eye = lax.broadcasted_iota(jnp.int32, (SEQ, SEQ), 0) == lax.broadcasted_iota(jnp.int32, (SEQ, SEQ), 1)
    for cc in range(NC):
        for xx in range(NX):
            for yy in range(NY):
                row = targets[2 * yy + cc, pl.ds(xx, 1), :].astype(F32)
                col = jnp.sum(jnp.where(eye, row, 0.0), axis=1, keepdims=True)
                tcol[pl.ds(((cc * NX + xx) * NY + yy) * SEQ, SEQ), :] = col

    @pl.loop(1, WAVES + 6)
    def _(i):
        @pl.when(i < WAVES)
        def _():
            z_in(i)
            z_on(i)
            s1(hab, slot(i), wa, i)

        @pl.when(i == 1)
        def _():
            s2(hc, z, wc, LAST)

        @pl.when((i >= 1) & (i < WAVES + 1))
        def _():
            s2(hab, slot(i - 1), wa, i - 1)

        @pl.when(i == 2)
        def _():
            s3(hc, z, wc, LAST)

        @pl.when((i >= 2) & (i < WAVES + 2))
        def _():
            s3(hab, slot(i - 2), wa, i - 2)

        @pl.when(i == 3)
        def _():
            s4(hc, z, wc, LAST)

        @pl.when((i >= 3) & (i < WAVES + 3))
        def _():
            s4(hab, slot(i - 3), wa, i - 3)

        @pl.when(i == 4)
        def _():
            s5(hc, z, wc, LAST)
            t1()
            thin_over(0)
            for k in range(NZ):
                weights(k).wait()

        @pl.when((i >= 4) & (i < WAVES + 4))
        def _():
            j = i - 4
            s5(hab, slot(j), wa, j)
            push(hab.at[slot(j), c], ds.at[j], dr.at[j], partner)

        @pl.when(i == 5)
        def _():
            t_step(1, 0)
            thin_multiply(0)

        @pl.when((i >= 5) & (i < WAVES + 5))
        def _():
            j = i - 5
            got(hab.at[0, 0], ds.at[j], dr.at[j])
            multiply(hab, slot(j), 0, WIDE)

        @pl.when(i == 6)
        def _():
            t_step(1, 1)
            thin_over(1)

        @pl.when(i == 7)
        def _():
            t_step(2, 0)
            thin_multiply(1)

        @pl.when(i == 8)
        def _():
            t_step(2, 1)
            thin_over(2)

        @pl.when(i == 9)
        def _():
            t_step(3, 0)
            thin_multiply(2)

        @pl.when(i == 10)
        def _():
            t_step(3, 1)
            thin_over(3)

        @pl.when(i == 11)
        def _():
            thin_multiply(3)

        @pl.when(i == 12)
        def _():
            t_in(4, 0)
            thin_over(4)
            thin_multiply(4)

    offset = (((aa * NX + x) * NZ + z) * vocab).astype(F32)
    lane = lax.broadcasted_iota(jnp.int32, (128, vocab), 1).astype(F32) + offset
    which = lax.broadcasted_iota(jnp.int32, (128, 128), 1)

    @pl.loop(0, NC * NX)
    def _(r):
        rows = pl.ds(pl.multiple_of(r * 128, 128), 128)
        logits = acc[rows, :]
        top = jnp.max(logits, axis=1, keepdims=True)
        total = jnp.sum(jnp.exp(logits - top), axis=1, keepdims=True)
        picked = jnp.sum(jnp.where(lane == tcol[rows, :], logits, 0.0), axis=1, keepdims=True)
        packed = jnp.where(which == 0, top, jnp.where(which == 1, total, jnp.where(which == 2, picked, 0.0)))
        stat[r] = packed.T[0:8]

    def merged(ref):
        tops, totals, picks = ref[:, 0:1, :], ref[:, 1:2, :], ref[:, 2:3, :]
        top = jnp.max(tops, axis=0)
        total = jnp.sum(jnp.exp(tops - top[None]) * totals, axis=0)
        return top, total, jnp.sum(picks, axis=0)

    me = (c * NX + x) * NY + y
    for n in range(1, NC * NX * NY):
        peer = (me + n) % (NC * NX * NY)
        group, py = peer // NY, peer % NY
        copy(stat.at[group], gath.at[me], es.at[0], er.at[0],
             at(group % NX, py, z, group // NX)).start()
    gath[me] = stat[c * NX + x]
    got(gath.at[pl.ds(0, NC * NX * NY - 1)], es.at[0], er.at[0])
    top, total, picked = merged(gath)
    zst[z] = jnp.concatenate([top, total, picked, jnp.zeros((5, 128), F32)], axis=0)
    for n in range(1, NZ):
        push(zst.at[z], es.at[1], er.at[1], at(x, y, (z + n) % NZ, c))
    got(zst.at[pl.ds(0, NZ - 1)], es.at[1], er.at[1])
    top, total, picked = merged(zst)
    logprob = picked - top - jnp.log(total)
    length = lengths[aa, x]
    spot = lax.broadcasted_iota(jnp.int32, (1, 128), 1) - y * SEQ
    live = (spot >= 0) & (spot < length)
    out[...] = jnp.sum(jnp.where(live, logprob, 0.0), axis=1, keepdims=True) / length.astype(F32)

    @pl.loop(0, WAVES)
    def _(j):
        s_done(hab, wa, j)
        sent(hab.at[0, 0], ds.at[j], dr.at[j])

        @pl.when(j > 0)
        def _():
            sent(hab.at[0, 0, 0, 0], zs.at[j], zr.at[j])

    s_done(hc, wc, LAST)
    for k in range(3):
        for q in range(2):
            sent(hc.at[0, 0], ts.at[k, q], tr.at[k, q])
    sent(hc.at[0, 0], ts.at[3, 0], tr.at[3, 0])
    for k in range(5):
        sent(thin_bytes(k), cs.at[k], cr.at[k])
    sent(gath.at[pl.ds(0, NC * NX * NY - 1)], es.at[0], er.at[0])
    sent(zst.at[pl.ds(0, NZ - 1)], es.at[1], er.at[1])


def body(hidden, unembed, targets, lengths):
    depth, vocab = unembed.shape
    rows = NC * NX * NY * SEQ
    dma = pltpu.SemaphoreType.DMA
    return pl.pallas_call(
        kernel,
        out_shape=jax.ShapeDtypeStruct((1, 1), F32),
        in_specs=[
            pl.BlockSpec(memory_space=pl.ANY),
            pl.BlockSpec(memory_space=pl.ANY),
            pl.BlockSpec(memory_space=pltpu.VMEM),
            pl.BlockSpec(memory_space=pltpu.SMEM),
        ],
        out_specs=pl.BlockSpec(memory_space=pltpu.VMEM),
        scratch_shapes=[
            pltpu.VMEM((NZ, NC, NX, NY, SEQ, WIDE), BF16),
            pltpu.VMEM((NZ, NC, NX, NY, SEQ, THIN), BF16),
            pltpu.VMEM((NZ, depth // NZ, vocab), BF16),
            pltpu.VMEM((rows, vocab), F32),
            pltpu.VMEM((rows, 1), F32),
            pltpu.VMEM((NC * NX, 8, 128), F32),
            pltpu.VMEM((NC * NX * NY, 8, 128), F32),
            pltpu.VMEM((NZ, 8, 128), F32),
            dma((2,)), dma((NZ,)),
            dma((WAVES,)), dma((WAVES,)),
            dma((WAVES + 1, 4)), dma((WAVES + 1, 4)),
            dma((4, 2)), dma((4, 2)),
            dma((WAVES,)), dma((WAVES,)),
            dma((5,)), dma((5,)),
            dma((2,)), dma((2,)),
        ],
        compiler_params=pltpu.CompilerParams(
            collective_id=0, has_side_effects=True, vmem_limit_bytes=60 << 20
        ),
    )(hidden, unembed, targets, lengths)


def solution(mesh):
    assert dict(mesh.shape) == {"aa": NY * NC, "ba": NX, "col": NZ}
    in_specs = (P("aa", "ba", None, "col"), P(None, ("aa", "ba", "col")), P(), P())
    return jax.shard_map(body, mesh=mesh, in_specs=in_specs, out_specs=P("aa", "ba"), check_vma=False)
```
